512 devices in a mesh: groups: 2 (over y), expert: 32 (over z, core), hidden: 8 (over x).
Axes of the slice: x: 8, y: 2, z: 16, core: 2. Of those that a mesh axis runs over, the one named last changes fastest.
The devices are a block of a 8x8x16 slice.
Arguments:
- tokens: bfloat16 [4096, 4096], P(('groups', 'expert'), 'hidden'), parts along dimension 0, may hold values from -6 to 6
- norm_gain: bfloat16 [4096], P('hidden'), may hold values from 0.25 to 1.75
- gate_proj: bfloat16 [64, 768, 4096], P('expert', 'hidden'), may hold values from -0.09375 to 0.09375
- up_proj: bfloat16 [64, 768, 4096], P('expert', 'hidden'), may hold values from -0.09375 to 0.09375
- down_proj: bfloat16 [64, 768, 4096], P('expert', 'hidden'), may hold values from -0.21875 to 0.21875
- expert_ids: int32 [4096, 8], P(('groups', 'expert')), parts along dimension 0, may hold values from 0 to 63, as said below
- slot_ids: int32 [4096, 8], P(('groups', 'expert')), parts along dimension 0, may hold values from 0 to 11, as said below
- gate_num: int32 [4096, 8], P(('groups', 'expert')), parts along dimension 0, may hold values from 1 to 255
Outputs:
- layer_out: bfloat16 [4096, 4096], P(('groups', 'expert'), 'hidden'), parts along dimension 0
The draws below stay inside these ranges and needn't reach their ends.
There are 2 independent parts, one for each index of `groups`. The reference program is written for one: setup_inputs(seed, part) draws one part's arguments, and reference() takes and returns one part's arrays. A program takes and returns all parts, laid end to end along the dimension named above; an argument that names none is the same for every part. Nothing has to cross between parts.
Inputs may be any that keep to these rules, and one draw needn't show every extreme that they name: `expert_ids`: each token names 8 different experts. In every aligned block of 64 tokens (the tokens of one index of the expert axis), a quarter of the experts are named by exactly 12 tokens, a quarter by 8 and the other half by 6; some expert is named by 12 tokens in every block. `slot_ids`: within an aligned block of 64 tokens, the routes that name one expert carry the slots 0 up to their count minus 1, each once.
All inputs are finite; a program needn't handle non-finite values.
Results may differ from the reference program's by a relative error of at most 0.0085.
Values may be sent and summed in bfloat16 or wider, within the bound.
No kernel may reach another device: no remote copies, remote signals or barrier semaphores. Data moves between devices by JAX's collectives and lax.ppermute only.
A program may use at most 64 MiB of HBM per device.

```python
import jax
import jax.numpy as jnp
import numpy as np
from jax import lax

D = 4096
HID = 768
SPECIALIST_COUNT = 64
TOPK = 8
TOK_SRC = 64
CAP = 12
HID_DEV = 96
TOKENS = 2048
N_EXPERT = 32
N_HIDDEN = 8


def route_layout(key):
    blocks = TOKENS // TOK_SRC
    prior_router_scores = jax.random.fold_in(key, 11)
    favoured_draw_seed, extra_draw_seed, jitter_draw_seed, sequence_draw_seed = jax.random.split(prior_router_scores, 4)
    labels = jnp.arange(SPECIALIST_COUNT, dtype=jnp.int32)
    hottest = jax.random.randint(favoured_draw_seed, (), 0, SPECIALIST_COUNT)
    specialist_extras = jax.random.randint(extra_draw_seed, (SPECIALIST_COUNT,), 0, 3) * (1 << 20)
    specialist_extras = jnp.where(labels == hottest, 3 * (1 << 20), specialist_extras)
    jitter = jax.random.randint(jitter_draw_seed, (blocks, SPECIALIST_COUNT), 0, 1 << 20)
    scores = (jitter + specialist_extras[None, :]) * SPECIALIST_COUNT + labels[None, :]
    ranked = jnp.argsort(-scores, axis=1).astype(jnp.int32)
    counts = np.array([CAP] * (SPECIALIST_COUNT // 4) + [2 * CAP // 3] * (SPECIALIST_COUNT // 4) + [CAP // 2] * (SPECIALIST_COUNT - SPECIALIST_COUNT // 2))
    starts = np.concatenate([np.zeros(1, np.int64), np.cumsum(counts)[:-1]])
    rank_of = np.repeat(np.arange(SPECIALIST_COUNT), counts)
    slot_of = np.arange(TOPK * TOK_SRC) - starts[rank_of]
    order_scores = jax.random.randint(sequence_draw_seed, (blocks, TOK_SRC), 0, 1 << 20) * TOK_SRC + jnp.arange(TOK_SRC, dtype=jnp.int32)[None, :]
    placement = jnp.argsort(order_scores, axis=1).astype(jnp.int32)
    position = jnp.arange(TOPK, dtype=jnp.int32)[None, None, :] * TOK_SRC + placement[:, :, None]
    rank_table = jnp.asarray(rank_of, dtype=jnp.int32)
    slot_table = jnp.asarray(slot_of, dtype=jnp.int32)
    ranks = rank_table[position].reshape(blocks, TOK_SRC * TOPK)
    chosen = jnp.take_along_axis(ranked, ranks, axis=1)
    slots = slot_table[position]
    return (chosen.reshape(TOKENS, TOPK).astype(jnp.int32), slots.reshape(TOKENS, TOPK).astype(jnp.int32))


def draw_expert_ids(key, part):
    return route_layout(key)[0]


def draw_slot_ids(key, part):
    return route_layout(key)[1]


def with_ends(entries, rng, low, top_value):
    longest = entries.shape.index(max(entries.shape))
    spots = []
    for shift in (0, 1):
        where = [jax.random.randint(jax.random.fold_in(rng, axis), (), 0, length) for axis, length in enumerate(entries.shape)]
        where[longest] = (where[longest] + shift) % entries.shape[longest]
        spots.append(tuple(where))
    return entries.at[spots[0]].set(low).at[spots[1]].set(top_value)


def strengthened(result, rng, source, target, blocks, factor):
    owner, partner = [(jnp.arange(result.shape[dim]) // (result.shape[dim] // blocks)).reshape([-1 if axis == dim else 1 for axis in range(result.ndim)]) for dim in (source, target)]
    chosen = jax.random.permutation(rng, blocks)[partner]
    strong = (owner == chosen) | (owner == (partner + blocks // 2) % blocks)
    return jnp.where(strong, factor * result, result)


def shard_levels(rng, dims, pieces, low, top_value):
    def one(dim, blocks):
        heights = jax.random.uniform(jax.random.fold_in(jax.random.fold_in(rng, 6), dim), (blocks,), jnp.float32, low / len(pieces), top_value / len(pieces))
        return jnp.repeat(jnp.exp(heights), dims[dim] // blocks).reshape((-1,) + (1,) * (len(dims) - dim - 1))

    level = one(*pieces[0])
    for cut in pieces[1:]:
        level = level * one(*cut)
    return level


def normal_values(rng, dims, deviation, limit, cuts=(), held_as=jnp.bfloat16):
    entries = jax.random.normal(rng, dims, jnp.float32) * deviation
    if len(cuts) > 0:
        entries = shard_levels(rng, dims, cuts, -0.22, 0.18) * entries
    return jnp.clip(entries, min=-limit, max=limit).astype(held_as)


def bell_draw_with(rng, dims, scale, reach, cuts, heavy, kind=jnp.bfloat16):
    drawn = scale * jax.random.normal(rng, dims, jnp.float32)
    if cuts:
        drawn = drawn * shard_levels(rng, dims, cuts, -0.22, 0.18)
    return jnp.clip(strengthened(drawn, jax.random.fold_in(rng, 3), *heavy), -reach, reach).astype(kind)


def setup_inputs(seed: int = 0, part: int = 0) -> dict:
    streams_of = jax.random.split(jax.random.key(seed), 9)
    part_splits = jax.random.split(jax.random.fold_in(streams_of[8], part), 9)
    return {
        "tokens": bell_draw_with(part_splits[0], (TOKENS, D), 1.0, 6.0, ((0, 32), (1, 8)), (1, 0, 32, 2.75)),
        "norm_gain": jnp.clip(1.0 + 0.15 * jax.random.normal(streams_of[1], (D,), jnp.float32), 0.25, 1.75).astype(jnp.bfloat16),
        "gate_proj": normal_values(streams_of[2], (SPECIALIST_COUNT, HID, D), D ** -0.5, 0.09375, ((0, 32), (1, 8))),
        "up_proj": normal_values(streams_of[3], (SPECIALIST_COUNT, HID, D), D ** -0.5, 0.09375, ((0, 32), (1, 8))),
        "down_proj": normal_values(streams_of[4], (SPECIALIST_COUNT, HID, D), HID ** -0.5, 0.21875, ((0, 32), (1, 8))),
        "expert_ids": draw_expert_ids(jax.random.fold_in(jax.random.fold_in(streams_of[8], part), 71), part),
        "slot_ids": draw_slot_ids(jax.random.fold_in(jax.random.fold_in(streams_of[8], part), 71), part),
        "gate_num": with_ends(jax.random.randint(part_splits[7], (TOKENS, TOPK), 1, 256), jax.random.fold_in(part_splits[7], 1), 1, 255).astype(jnp.int32),
    }


gate_scale = 1.0 / 1024.0

def expert_block(operands):
    inputs, gate_weight, up_weight, down_weight = operands
    flat_rows = inputs.reshape(-1, D)
    gate_act = jnp.dot(flat_rows, gate_weight.T, preferred_element_type=jnp.float32)
    up_act = jnp.dot(flat_rows, up_weight.T, preferred_element_type=jnp.float32)
    activated = (jax.nn.silu(gate_act) * up_act).astype(jnp.bfloat16)
    split_act = activated.reshape(-1, N_HIDDEN, HID_DEV).astype(jnp.float32)
    split_down = down_weight.reshape(N_HIDDEN, HID_DEV, D).astype(jnp.float32)
    partials = jnp.einsum('rjh,jhd->jrd', split_act, split_down).astype(jnp.bfloat16)
    partials = lax.optimization_barrier(partials)
    return lax.optimization_barrier(jnp.sum(partials.astype(jnp.float32), axis=0)).reshape(N_EXPERT, CAP, D)

def reference(tokens, norm_gain, gate_proj, up_proj, down_proj, expert_ids, slot_ids, gate_num):
    features = tokens.astype(jnp.float32)
    squares = lax.optimization_barrier(jnp.sum(features * features, axis=1))
    scale = lax.rsqrt(squares / D + 0.5)
    normed = (features * scale[:, None] * norm_gain.astype(jnp.float32)[None, :]).astype(jnp.bfloat16)
    source = (jnp.arange(TOKENS) // TOK_SRC).astype(jnp.int32)
    buffer = jnp.zeros((SPECIALIST_COUNT, N_EXPERT, CAP, D), jnp.bfloat16)
    spread_rows = jnp.broadcast_to(normed[:, None, :], (TOKENS, TOPK, D))
    buffer = buffer.at[expert_ids, source[:, None], slot_ids].set(spread_rows)
    expert_out = lax.map(expert_block, (buffer, gate_proj, up_proj, down_proj))
    picked = expert_out[expert_ids, source[:, None], slot_ids]
    gates = gate_num.astype(jnp.float32) * gate_scale
    return lax.optimization_barrier(jnp.sum(picked * gates[:, :, None], axis=1)).astype(jnp.bfloat16)
```

```python
import jax
import jax.numpy as jnp
from jax import lax
from jax.sharding import Mesh
from jax.sharding import PartitionSpec as P

CAP = 12
EXPERT = ("expert_0", "expert_1")
GROUPS_EXPERT = ("groups", "expert_0", "expert_1")


gate_scale = 1.0 / 1024.0


def shifted(array, step):
    devices = lax.axis_size("hidden")
    return lax.ppermute(array, "hidden", [(i, (i + step) % devices) for i in range(devices)])


def feature_block(weights, index, width):
    return lax.dynamic_slice_in_dim(weights, index * width, width, axis=weights.ndim - 1)


def exchange_in_order(tiles, axes, order):
    shape = [lax.axis_size(a) for a in axes]
    tiles = tiles.reshape(*shape, *tiles.shape[1:])
    for k in order:
        tiles = lax.all_to_all(tiles, axes[k], split_axis=k, concat_axis=k, tiled=True)
    return tiles.reshape(-1, *tiles.shape[len(axes) :])


def route_tables(expert_ids, slot_ids, gate_num, slots):
    slot_index = expert_ids * CAP + slot_ids
    columns = lax.broadcasted_iota(jnp.int32, (1, 1, slots), 2)
    matches = slot_index[:, :, None] == columns
    placing = jnp.any(matches, axis=1).astype(jnp.bfloat16)
    scaled = gate_num.astype(jnp.float32) * gate_scale
    weights = jnp.sum(jnp.where(matches, scaled[:, :, None], 0.0), axis=1).astype(jnp.bfloat16)
    return (placing, weights)


def on_device(tokens, norm_gain, gate_proj, up_proj, down_proj, expert_ids, slot_ids, gate_num):
    parts = lax.axis_size("hidden")
    here = lax.axis_index("hidden")
    sources = lax.axis_size(EXPERT)
    local, units, features = gate_proj.shape
    width = tokens.shape[1]
    per_source = local * CAP
    rows_all = sources * per_source

    gain_rows = jnp.broadcast_to(norm_gain[None, :], (8, width))
    down_by_shift = []
    for d in range(parts):
        cut = feature_block(down_proj, (here + d) % parts, width).reshape(local * units, width)
        if d:
            got = shifted(jnp.concatenate([cut, gain_rows], axis=0), d)
            down_by_shift.append((got[: local * units], got[local * units]))
        else:
            down_by_shift.append((cut, norm_gain))

    placing, weights = route_tables(expert_ids, slot_ids, gate_num, rows_all)
    outgoing = lax.dot_general(
        placing, tokens, (((0,), (0,)), ((), ())), preferred_element_type=jnp.float32
    ).astype(jnp.bfloat16)
    received = exchange_in_order(outgoing.reshape(sources, per_source, width), EXPERT, (1, 0))
    received = received.reshape(rows_all, width)

    blocks = {0: received}
    ahead = back = received
    full = (parts - 1) // 2
    for s in range(1, full + 1):
        ahead = shifted(ahead, 1)
        back = shifted(back, -1)
        blocks[s] = ahead
        blocks[parts - s] = back
    half = rows_all // 2
    blocks[full + 1] = jnp.concatenate(
        [shifted(ahead[:half], 1), shifted(back[half:], -1)], axis=0
    )

    order = [0]
    for s in range(1, full + 1):
        order += [s, parts - s]
    order.append(full + 1)
    both = jnp.zeros((2 * local * units, rows_all), jnp.float32)
    squares = jnp.zeros((rows_all,), jnp.float32)
    for d in order:
        index = (here - d + parts) % parts
        cut = jnp.concatenate(
            [
                feature_block(w, index, width).reshape(local * units, width)
                for w in (gate_proj, up_proj)
            ],
            axis=0,
        )
        gain = down_by_shift[d][1].astype(jnp.float32)
        cut = (cut.astype(jnp.float32) * gain[None, :]).astype(jnp.bfloat16)
        both = both + lax.dot_general(
            cut, blocks[d], (((1,), (1,)), ((), ())), preferred_element_type=jnp.float32
        )
        squares = squares + jnp.sum(jnp.square(blocks[d].astype(jnp.float32)), axis=1)

    scale = lax.rsqrt(squares / features + 0.5)
    both = both.reshape(2, local, units, rows_all) * scale
    owner = (lax.broadcasted_iota(jnp.int32, (1, rows_all), 1) % per_source) // CAP
    own = both[:, 0]
    for e in range(1, local):
        own = jnp.where(owner == e, both[:, e], own)
    activated = (jax.nn.silu(own[0]) * own[1]).astype(jnp.bfloat16)

    result = jnp.zeros((rows_all, width), jnp.float32)
    for d in range(parts):
        act = shifted(activated, d) if d else activated
        spread = jnp.concatenate(
            [jnp.where(owner == e, act, jnp.zeros_like(act)) for e in range(local)], axis=0
        )
        result = result + lax.dot_general(
            spread, down_by_shift[d][0], (((0,), (0,)), ((), ())), preferred_element_type=jnp.float32
        )

    returned = exchange_in_order(
        result.astype(jnp.bfloat16).reshape(sources, per_source, width), EXPERT, (1, 0)
    )
    combined = jnp.dot(
        weights, returned.reshape(rows_all, width), preferred_element_type=jnp.float32
    )
    return combined.astype(jnp.bfloat16)


def solution(mesh):
    torus = Mesh(
        mesh.devices.reshape(
            mesh.shape["groups"], mesh.shape["expert"] // 2, 2, mesh.shape["hidden"]
        ),
        ("groups", "expert_0", "expert_1", "hidden"),
    )
    in_specs = (
        P(GROUPS_EXPERT, "hidden"),
        P("hidden"),
        P(EXPERT, "hidden", None),
        P(EXPERT, "hidden", None),
        P(EXPERT, "hidden", None),
        P(GROUPS_EXPERT, None),
        P(GROUPS_EXPERT, None),
        P(GROUPS_EXPERT, None),
    )
    out_specs = P(GROUPS_EXPERT, "hidden")
    return jax.shard_map(
        on_device, mesh=torus, in_specs=in_specs, out_specs=out_specs, check_vma=False
    )
```

```python
import jax
import jax.numpy as jnp
from jax import lax
from jax.sharding import Mesh
from jax.sharding import PartitionSpec as P
from jax.experimental import pallas as pl
from jax.experimental.pallas import tpu as pltpu

EXPERT = ("expert_0", "expert_1")
GROUPS_EXPERT = ("groups", "expert_0", "expert_1")
CHUNKS = ((0, 8), (8, 12))


gate_scale = 1.0 / 1024.0


def shifted(array, step):
    devices = lax.axis_size("hidden")
    return lax.ppermute(array, "hidden", [(i, (i + step) % devices) for i in range(devices)])


def feature_block(weights, index, width):
    return lax.dynamic_slice_in_dim(weights, index * width, width, axis=weights.ndim - 1)


def put_in_hbm(array):
    def copy(src, dst, sem):
        move = pltpu.make_async_copy(src, dst, sem)
        move.start()
        move.wait()

    return pl.pallas_call(
        copy,
        out_shape=jax.ShapeDtypeStruct(array.shape, array.dtype),
        in_specs=[pl.BlockSpec(memory_space=pltpu.VMEM)],
        out_specs=pl.BlockSpec(memory_space=pltpu.HBM),
        scratch_shapes=[pltpu.SemaphoreType.DMA],
        cost_estimate=pl.CostEstimate(
            flops=0, bytes_accessed=2 * array.size * array.dtype.itemsize, transcendentals=0
        ),
    )(array)


def sent(tiles, axes):
    return lax.all_to_all(tiles, axes, split_axis=0, concat_axis=0, tiled=True)


def route_tables(expert_ids, slot_ids, gate_num, slots, low, high):
    span = high - low
    inside = (slot_ids >= low) & (slot_ids < high)
    slot_index = jnp.where(inside, expert_ids * span + (slot_ids - low), -1)
    columns = lax.broadcasted_iota(jnp.int32, (1, 1, slots), 2)
    matches = slot_index[:, :, None] == columns
    placing = jnp.any(matches, axis=1).astype(jnp.bfloat16)
    scaled = gate_num.astype(jnp.float32) * gate_scale
    weights = jnp.sum(jnp.where(matches, scaled[:, :, None], 0.0), axis=1).astype(jnp.bfloat16)
    return (placing, weights)


def layer(tokens, norm_gain, gate_proj, up_proj, down_proj, expert_ids, slot_ids, gate_num):
    parts = lax.axis_size("hidden")
    here = lax.axis_index("hidden")
    sources = lax.axis_size(EXPERT)
    local, units, features = gate_proj.shape
    width = tokens.shape[1]
    full = (parts - 1) // 2
    order = [0]
    for s in range(1, full + 1):
        order += [s, parts - s]
    order.append(full + 1)
    by_reach = order

    def dispatched(low, high, after):
        per_source = local * (high - low)
        placing, weights = route_tables(
            expert_ids, slot_ids, gate_num, sources * per_source, low, high
        )
        outgoing = lax.dot_general(
            placing, tokens, (((0,), (0,)), ((), ())), preferred_element_type=jnp.float32
        ).astype(jnp.bfloat16)
        if after is not None:
            outgoing, after = lax.optimization_barrier((outgoing, after))
        received = sent(put_in_hbm(outgoing.reshape(sources, per_source, width)), EXPERT)
        return received.reshape(-1, width), weights

    arrived = []
    for chunk in CHUNKS:
        arrived.append(dispatched(*chunk, arrived[-1][0] if arrived else None))

    down_rows = local * units
    gain_rows = jnp.broadcast_to(norm_gain[None, :], (8, width))
    down_by_shift = [None] * parts
    for d in by_reach:
        cut = feature_block(down_proj, (here + d) % parts, width).reshape(down_rows, width)
        cut = jnp.concatenate([cut, gain_rows], axis=0)
        down_by_shift[d] = shifted(cut, d) if d else cut

    weights_by_shift = []
    for d in range(parts):
        index = (here - d + parts) % parts
        cut = jnp.concatenate(
            [
                feature_block(w, index, width).reshape(local * units, width)
                for w in (gate_proj, up_proj)
            ],
            axis=0,
        )
        gain = down_by_shift[d][down_rows]
        weights_by_shift.append(
            (cut.astype(jnp.float32) * gain.astype(jnp.float32)[None, :]).astype(jnp.bfloat16)
        )

    def hidden_units(received, per_source, after):
        rows_all = received.shape[0]
        if after is not None:
            received, after = lax.optimization_barrier((received, after))
        blocks = {0: received}
        ahead = back = received
        for s in range(1, full + 1):
            ahead = shifted(ahead, 1)
            back = shifted(back, -1)
            blocks[s] = ahead
            blocks[parts - s] = back
        half = rows_all // 2
        blocks[full + 1] = jnp.concatenate(
            [shifted(ahead[:half], 1), shifted(back[half:], -1)], axis=0
        )
        both = jnp.zeros((2 * local * units, rows_all), jnp.float32)
        squares = jnp.zeros((rows_all,), jnp.float32)
        for d in order:
            both = both + lax.dot_general(
                weights_by_shift[d],
                blocks[d],
                (((1,), (1,)), ((), ())),
                preferred_element_type=jnp.float32,
            )
            squares = squares + jnp.sum(jnp.square(blocks[d].astype(jnp.float32)), axis=1)
        scale = lax.rsqrt(squares / features + 0.5)
        both = both.reshape(2, local, units, rows_all) * scale
        span = per_source // local
        owner = (lax.broadcasted_iota(jnp.int32, (1, rows_all), 1) % per_source) // span
        own = both[:, 0]
        for e in range(1, local):
            own = jnp.where(owner == e, both[:, e], own)
        return (jax.nn.silu(own[0]) * own[1]).astype(jnp.bfloat16), owner, (ahead, back)

    def finished(activated, owner, per_source, after):
        rows_all = activated.shape[1]
        result = jnp.zeros((rows_all, width), jnp.float32)
        for d in by_reach:
            act = shifted(activated, d) if d else activated
            spread = jnp.concatenate(
                [jnp.where(owner == e, act, jnp.zeros_like(act)) for e in range(local)], axis=0
            )
            result = result + lax.dot_general(
                spread,
                down_by_shift[d][:down_rows],
                (((0,), (0,)), ((), ())),
                preferred_element_type=jnp.float32,
            )
        tiles = put_in_hbm(result.astype(jnp.bfloat16).reshape(sources, per_source, width))
        if after is not None:
            tiles, after = lax.optimization_barrier((tiles, after))
        return tiles, sent(tiles, EXPERT).reshape(rows_all, width)

    combined = jnp.zeros(tokens.shape, jnp.float32)
    after = tiles = returned = None
    for (low, high), (received, weights) in zip(CHUNKS, arrived):
        per_source = local * (high - low)
        activated, owner, after = hidden_units(received, per_source, after)
        if tiles is not None:
            activated, tiles = lax.optimization_barrier((activated, tiles))
        tiles, returned = finished(activated, owner, per_source, returned)
        combined = combined + jnp.dot(weights, returned, preferred_element_type=jnp.float32)
    return combined.astype(jnp.bfloat16)


def solution(mesh):
    torus = Mesh(
        mesh.devices.reshape(
            mesh.shape["groups"], mesh.shape["expert"] // 2, 2, mesh.shape["hidden"]
        ),
        ("groups", "expert_0", "expert_1", "hidden"),
    )
    in_specs = (
        P(GROUPS_EXPERT, "hidden"),
        P("hidden"),
        P(EXPERT, "hidden", None),
        P(EXPERT, "hidden", None),
        P(EXPERT, "hidden", None),
        P(GROUPS_EXPERT, None),
        P(GROUPS_EXPERT, None),
        P(GROUPS_EXPERT, None),
    )
    out_specs = P(GROUPS_EXPERT, "hidden")
    return jax.shard_map(layer, mesh=torus, in_specs=in_specs, out_specs=out_specs, check_vma=False)
```

```python
import jax
import jax.numpy as jnp
from jax import lax
from jax.experimental import pallas as pl
from jax.experimental.pallas import tpu as pltpu
from jax.sharding import Mesh
from jax.sharding import PartitionSpec as P

CAP = 12
HALVES = 2
LIMIT = 20 * 2**20
EXPERT = ("expert_0", "expert_1")
GROUPS_EXPERT = ("groups", "expert_0", "expert_1")


gate_scale = 1.0 / 1024.0


def shifted(array, step):
    devices = lax.axis_size("hidden")
    return lax.ppermute(array, "hidden", [(i, (i + step) % devices) for i in range(devices)])


def feature_block(weights, index, width):
    return lax.dynamic_slice_in_dim(weights, index * width, width, axis=weights.ndim - 1)


def sent(tiles, axes):
    return lax.all_to_all(tiles, axes, split_axis=0, concat_axis=0, tiled=True)


def in_two_stages(tiles):
    shape = [lax.axis_size(a) for a in EXPERT]
    tiles = tiles.reshape(*shape, *tiles.shape[1:])
    for k in (1, 0):
        tiles = lax.all_to_all(tiles, EXPERT[k], split_axis=k, concat_axis=k, tiled=True)
    return tiles


def route_tables(expert_ids, slot_ids, gate_num, slots):
    slot_index = expert_ids * CAP + slot_ids
    columns = lax.broadcasted_iota(jnp.int32, (1, 1, slots), 2)
    matches = slot_index[:, :, None] == columns
    placing = jnp.any(matches, axis=1).astype(jnp.bfloat16)
    scaled = gate_num.astype(jnp.float32) * gate_scale
    weights = jnp.sum(jnp.where(matches, scaled[:, :, None], 0.0), axis=1).astype(jnp.bfloat16)
    return (placing, weights)


def unpacked(turns, pieces, parts, rows, width):
    arrays = []
    for _, array, *_ in pieces:
        if not any(array is known for known in arrays):
            arrays.append(array)

    def place(array):
        return [array is known for known in arrays].index(True)

    def body(turn, *refs):
        sources, (down, gains, sems) = refs[: len(arrays)], refs[len(arrays) :]
        moves = []
        for n, (d, array, low, at, count) in enumerate(pieces):
            target = gains.at[d] if at is None else down.at[turn[d], pl.ds(at, count)]
            source = sources[place(array)].at[pl.ds(low, count)]
            moves.append(pltpu.make_async_copy(source, target, sems.at[n]))
        for move in moves:
            move.start()
        for move in moves:
            move.wait()

    vmem = pl.BlockSpec(memory_space=pltpu.VMEM)
    return pl.pallas_call(
        body,
        out_shape=[
            jax.ShapeDtypeStruct((parts, rows, width), jnp.bfloat16),
            jax.ShapeDtypeStruct((parts, 8, width), jnp.bfloat16),
        ],
        in_specs=[pl.BlockSpec(memory_space=pltpu.SMEM)]
        + [pl.BlockSpec(memory_space=pltpu.HBM)] * len(arrays),
        out_specs=[vmem] * 2,
        scratch_shapes=[pltpu.SemaphoreType.DMA((len(pieces),))],
        compiler_params=pltpu.CompilerParams(vmem_limit_bytes=LIMIT),
        cost_estimate=pl.CostEstimate(
            flops=10**8, bytes_accessed=4 * parts * rows * width, transcendentals=0
        ),
    )(turns, *arrays)


def add_blocks(turns, gate_proj, up_proj, gains, blocks, before, finish):
    local, units, features = gate_proj.shape
    parts, _, width = gains.shape
    count = len(blocks)
    pieces = [piece for group in blocks.values() for piece in group]
    rows_all = sum(piece.shape[0] for piece in pieces) // count
    wide = 2 * local * units
    shapes = [
        jax.ShapeDtypeStruct((wide, rows_all), jnp.float32),
        jax.ShapeDtypeStruct((rows_all, 128), jnp.float32),
    ]

    def body(turn, gate, up, gain_ref, *refs):
        block_refs, refs = list(refs[: len(pieces)]), refs[len(pieces) :]
        start_sums, start_squares = refs[:2] if before else (None, None)
        refs = refs[2:] if before else refs
        out, (sums, squares) = (refs[0], refs[1:]) if finish else (None, refs)
        for n, (d, group) in enumerate(blocks.items()):
            start = pl.multiple_of(turn[d] * width, 128)
            cut = jnp.concatenate(
                [w[e, :, pl.ds(start, width)] for w in (gate, up) for e in range(local)], axis=0
            )
            cut = cut * gain_ref[d, 0:1, :]
            first = 0
            for piece in group:
                rows = block_refs.pop(0)[...]
                here = pl.ds(first, piece.shape[0])
                first += piece.shape[0]
                product = lax.dot_general(
                    cut, rows, (((1,), (1,)), ((), ())), preferred_element_type=jnp.float32
                )
                square = jnp.square(rows.astype(jnp.float32))
                square = sum(square[:, k : k + 128] for k in range(0, width, 128))
                if n or before:
                    old_sums, old_squares = (sums, squares) if n else (start_sums, start_squares)
                    product = product + old_sums[:, here]
                    square = square + old_squares[here, :]
                sums[:, here] = product
                squares[here, :] = square
        if finish:
            total = jnp.sum(squares[...].T, axis=0, keepdims=True)
            scale = lax.rsqrt(total / features + 0.5)
            owner = lax.broadcasted_iota(jnp.int32, (1, rows_all), 1) % (local * CAP) // CAP
            own = []
            for k in range(2):
                value = sums[pl.ds(k * local * units, units), :]
                for e in range(1, local):
                    other = sums[pl.ds((k * local + e) * units, units), :]
                    value = jnp.where(owner == e, other, value)
                own.append(value * scale)
            done = (own[0] / (1.0 + jnp.exp(-own[0])) * own[1]).astype(jnp.bfloat16)
            for j in range(parts):
                out[j] = done

    vmem = pl.BlockSpec(memory_space=pltpu.VMEM)
    held = [] if before is None else list(before)
    done = jax.ShapeDtypeStruct((parts, units, rows_all), jnp.bfloat16)
    return pl.pallas_call(
        body,
        out_shape=done if finish else shapes,
        in_specs=[pl.BlockSpec(memory_space=pltpu.SMEM)] + [vmem] * (3 + len(pieces) + len(held)),
        out_specs=vmem if finish else [vmem] * 2,
        scratch_shapes=[pltpu.VMEM(s.shape, s.dtype) for s in shapes] if finish else [],
        compiler_params=pltpu.CompilerParams(vmem_limit_bytes=LIMIT),
        cost_estimate=pl.CostEstimate(
            flops=2 * wide * width * rows_all * count, bytes_accessed=0, transcendentals=0
        ),
    )(turns, gate_proj, up_proj, gains, *pieces, *held)


def layer(tokens, norm_gain, gate_proj, up_proj, down_proj, expert_ids, slot_ids, gate_num):
    parts = lax.axis_size("hidden")
    here = lax.axis_index("hidden")
    sources = lax.axis_size(EXPERT)
    local, units, _ = gate_proj.shape
    width = tokens.shape[1]
    per_source = local * CAP
    rows_all = sources * per_source
    down_rows = local * units

    full = (parts - 1) // 2
    order = [0]
    for s in range(1, full + 1):
        order += [s, parts - s]
    order.append(full + 1)

    gain_rows = jnp.broadcast_to(norm_gain[None, :], (8, width))
    cuts = [
        feature_block(down_proj, (here + d) % parts, width).reshape(down_rows, width)
        for d in range(parts)
    ]
    far = full + 1
    kept = down_rows - units
    cut_by_shift = [jnp.concatenate([cut, gain_rows], axis=0) for cut in cuts]
    cut_by_shift[far] = jnp.concatenate([cuts[far][:kept], gain_rows], axis=0)
    one, three = parts - 1, parts - (far - 1)
    end = down_rows + 8
    first = shifted(jnp.concatenate([cut_by_shift[one], cuts[far][kept:]], axis=0), one)
    for d in range(1, parts):
        if d not in (one, three):
            cut_by_shift[d] = shifted(cut_by_shift[d], d)
    cut_by_shift[one] = first
    cut_by_shift[three] = shifted(
        jnp.concatenate([cut_by_shift[three], first[end:]], axis=0), three
    )
    turns = jnp.stack([(here - d + parts) % parts for d in range(parts)]).astype(jnp.int32)
    pieces = []
    for d, cut in enumerate(cut_by_shift):
        pieces.append((d, cut, 0, 0, kept if d == far else down_rows))
        pieces.append((d, cut, kept if d == far else down_rows, None, 8))
    pieces.append((far, cut_by_shift[three], end, kept, units))
    down_all, gains = unpacked(turns, pieces, parts, down_rows, width)

    placing, weights = route_tables(expert_ids, slot_ids, gate_num, rows_all)
    outgoing = lax.dot_general(
        placing, tokens, (((0,), (0,)), ((), ())), preferred_element_type=jnp.float32
    ).astype(jnp.bfloat16)
    received = in_two_stages(outgoing.reshape(sources, per_source, width))
    received = received.reshape(rows_all, width)

    size = rows_all // HALVES
    owner = (lax.broadcasted_iota(jnp.int32, (1, rows_all), 1) % per_source) // CAP
    halves = [received[k * size : (k + 1) * size] for k in range(HALVES)]
    blocks = [{0: half} for half in halves]
    ahead, back = list(halves), list(halves)
    for s in range(1, full + 1):
        for k in range(HALVES):
            ahead[k] = blocks[k][s] = shifted(ahead[k], 1)
            back[k] = blocks[k][parts - s] = shifted(back[k], -1)
    early = [d for d in order if min(d, parts - d) < full]
    held = add_blocks(
        turns, gate_proj, up_proj, gains, {d: [b[d] for b in blocks] for d in early}, None, False
    )
    ahead[0], back[1], held = lax.optimization_barrier((ahead[0], back[1], held))
    blocks[0][far] = shifted(ahead[0], 1)
    blocks[1][far] = shifted(back[1], -1)
    late = [d for d in order if d not in early]
    copies = add_blocks(
        turns, gate_proj, up_proj, gains, {d: [b[d] for b in blocks] for d in late}, held, True
    )
    held = (copies, down_all, weights, owner)
    copies, down_all, weights, owner = lax.optimization_barrier(held)
    gathered = sent(copies, "hidden")
    gathered = gathered.reshape(parts * units, rows_all)
    result = jnp.zeros((rows_all, width), jnp.float32)
    for e in range(local):
        spread = jnp.where(owner == e, gathered, jnp.zeros_like(gathered))
        down = down_all[:, e * units : (e + 1) * units].reshape(parts * units, width)
        result = result + lax.dot_general(
            spread, down, (((0,), (0,)), ((), ())), preferred_element_type=jnp.float32
        )

    tiles = result.astype(jnp.bfloat16).reshape(sources, per_source, width)
    returned = sent(tiles, EXPERT).reshape(rows_all, width)
    combined = jnp.dot(weights, returned, preferred_element_type=jnp.float32)
    return combined.astype(jnp.bfloat16)


def solution(mesh):
    torus = Mesh(
        mesh.devices.reshape(
            mesh.shape["groups"], mesh.shape["expert"] // 2, 2, mesh.shape["hidden"]
        ),
        ("groups", "expert_0", "expert_1", "hidden"),
    )
    in_specs = (
        P(GROUPS_EXPERT, "hidden"),
        P("hidden"),
        P(EXPERT, "hidden", None),
        P(EXPERT, "hidden", None),
        P(EXPERT, "hidden", None),
        P(GROUPS_EXPERT, None),
        P(GROUPS_EXPERT, None),
        P(GROUPS_EXPERT, None),
    )
    out_specs = P(GROUPS_EXPERT, "hidden")
    return jax.shard_map(layer, mesh=torus, in_specs=in_specs, out_specs=out_specs, check_vma=False)
```

```python
import jax
import jax.numpy as jnp
from jax import lax
from jax.experimental import pallas as pl
from jax.experimental.pallas import tpu as pltpu
from jax.sharding import Mesh
from jax.sharding import PartitionSpec as P

CAP = 12
HALVES = 2
LIMIT = 20 * 2**20
EXPERT = ("expert_0", "expert_1")
GROUPS_EXPERT = ("groups", "expert_0", "expert_1")


gate_scale = 1.0 / 1024.0


def shifted(array, step):
    devices = lax.axis_size("hidden")
    return lax.ppermute(array, "hidden", [(i, (i + step) % devices) for i in range(devices)])


def feature_block(weights, index, width):
    return lax.dynamic_slice_in_dim(weights, index * width, width, axis=weights.ndim - 1)


def sent(tiles, axes):
    return lax.all_to_all(tiles, axes, split_axis=0, concat_axis=0, tiled=True)


def route_tables(expert_ids, slot_ids, gate_num, slots):
    slot_index = expert_ids * CAP + slot_ids
    columns = lax.broadcasted_iota(jnp.int32, (1, 1, slots), 2)
    matches = slot_index[:, :, None] == columns
    placing = jnp.any(matches, axis=1).astype(jnp.bfloat16)
    scaled = gate_num.astype(jnp.float32) * gate_scale
    weights = jnp.sum(jnp.where(matches, scaled[:, :, None], 0.0), axis=1).astype(jnp.bfloat16)
    return (placing, weights)


def unpacked(turns, pieces, parts, rows, width):
    arrays = []
    for _, array, *_ in pieces:
        if not any(array is known for known in arrays):
            arrays.append(array)

    def place(array):
        return [array is known for known in arrays].index(True)

    def body(turn, *refs):
        sources, (down, gains, sems) = refs[: len(arrays)], refs[len(arrays) :]
        moves = []
        for n, (d, array, low, at, count) in enumerate(pieces):
            target = gains.at[d] if at is None else down.at[turn[d], pl.ds(at, count)]
            source = sources[place(array)].at[pl.ds(low, count)]
            moves.append(pltpu.make_async_copy(source, target, sems.at[n]))
        for move in moves:
            move.start()
        for move in moves:
            move.wait()

    vmem = pl.BlockSpec(memory_space=pltpu.VMEM)
    return pl.pallas_call(
        body,
        out_shape=[
            jax.ShapeDtypeStruct((parts, rows, width), jnp.bfloat16),
            jax.ShapeDtypeStruct((parts, 8, width), jnp.bfloat16),
        ],
        in_specs=[pl.BlockSpec(memory_space=pltpu.SMEM)]
        + [pl.BlockSpec(memory_space=pltpu.HBM)] * len(arrays),
        out_specs=[vmem] * 2,
        scratch_shapes=[pltpu.SemaphoreType.DMA((len(pieces),))],
        compiler_params=pltpu.CompilerParams(vmem_limit_bytes=LIMIT),
        cost_estimate=pl.CostEstimate(
            flops=10**8, bytes_accessed=4 * parts * rows * width, transcendentals=0
        ),
    )(turns, *arrays)


def add_blocks(turns, gate_proj, up_proj, gains, blocks, before, finish):
    local, units, features = gate_proj.shape
    parts, _, width = gains.shape
    count = len(blocks)
    pieces = [piece for group in blocks.values() for piece in group]
    rows_all = sum(piece.shape[0] for piece in pieces) // count
    wide = 2 * local * units
    shapes = [
        jax.ShapeDtypeStruct((wide, rows_all), jnp.float32),
        jax.ShapeDtypeStruct((rows_all, 128), jnp.float32),
    ]

    def body(turn, gate, up, gain_ref, *refs):
        block_refs, refs = list(refs[: len(pieces)]), refs[len(pieces) :]
        refs, (landed, sems) = refs[:-2], refs[-2:]
        moves = [
            pltpu.make_async_copy(ref, landed.at[n], sems.at[n]) for n, ref in enumerate(block_refs)
        ]
        for move in moves:
            move.start()
        done_pieces = 0
        start_sums, start_squares = refs[:2] if before else (None, None)
        refs = refs[2:] if before else refs
        out, (sums, squares) = (refs[0], refs[1:]) if finish else (None, refs)
        for n, (d, group) in enumerate(blocks.items()):
            start = pl.multiple_of(turn[d] * width, 128)
            cut = jnp.concatenate(
                [w[e, :, pl.ds(start, width)] for w in (gate, up) for e in range(local)], axis=0
            )
            cut = cut * gain_ref[d, 0:1, :]
            first = 0
            for piece in group:
                moves[done_pieces].wait()
                rows = landed[done_pieces]
                done_pieces += 1
                here = pl.ds(first, piece.shape[0])
                first += piece.shape[0]
                product = lax.dot_general(
                    cut, rows, (((1,), (1,)), ((), ())), preferred_element_type=jnp.float32
                )
                square = jnp.square(rows.astype(jnp.float32))
                square = sum(square[:, k : k + 128] for k in range(0, width, 128))
                if n or before:
                    old_sums, old_squares = (sums, squares) if n else (start_sums, start_squares)
                    product = product + old_sums[:, here]
                    square = square + old_squares[here, :]
                sums[:, here] = product
                squares[here, :] = square
        if finish:
            total = jnp.sum(squares[...].T, axis=0, keepdims=True)
            scale = lax.rsqrt(total / features + 0.5)
            owner = lax.broadcasted_iota(jnp.int32, (1, rows_all), 1) % (local * CAP) // CAP
            own = []
            for k in range(2):
                value = sums[pl.ds(k * local * units, units), :]
                for e in range(1, local):
                    other = sums[pl.ds((k * local + e) * units, units), :]
                    value = jnp.where(owner == e, other, value)
                own.append(value * scale)
            done = (own[0] / (1.0 + jnp.exp(-own[0])) * own[1]).astype(jnp.bfloat16)
            for j in range(parts):
                out[j] = done

    vmem = pl.BlockSpec(memory_space=pltpu.VMEM)
    held = [] if before is None else list(before)
    done = jax.ShapeDtypeStruct((parts, units, rows_all), jnp.bfloat16)
    return pl.pallas_call(
        body,
        out_shape=done if finish else shapes,
        in_specs=[pl.BlockSpec(memory_space=pltpu.SMEM)]
        + [vmem] * 3
        + [pl.BlockSpec(memory_space=pltpu.HBM)] * len(pieces)
        + [vmem] * len(held),
        out_specs=vmem if finish else [vmem] * 2,
        scratch_shapes=([pltpu.VMEM(s.shape, s.dtype) for s in shapes] if finish else [])
        + [
            pltpu.VMEM((len(pieces), *pieces[0].shape), pieces[0].dtype),
            pltpu.SemaphoreType.DMA((len(pieces),)),
        ],
        compiler_params=pltpu.CompilerParams(vmem_limit_bytes=LIMIT),
        cost_estimate=pl.CostEstimate(
            flops=2 * wide * width * rows_all * count, bytes_accessed=0, transcendentals=0
        ),
    )(turns, gate_proj, up_proj, gains, *pieces, *held)


def layer(tokens, norm_gain, gate_proj, up_proj, down_proj, expert_ids, slot_ids, gate_num):
    parts = lax.axis_size("hidden")
    here = lax.axis_index("hidden")
    sources = lax.axis_size(EXPERT)
    local, units, _ = gate_proj.shape
    width = tokens.shape[1]
    per_source = local * CAP
    rows_all = sources * per_source
    down_rows = local * units

    full = (parts - 1) // 2
    order = [0]
    for s in range(1, full + 1):
        order += [s, parts - s]
    order.append(full + 1)

    gain_rows = jnp.broadcast_to(norm_gain[None, :], (8, width))
    cuts = [
        feature_block(down_proj, (here + d) % parts, width).reshape(down_rows, width)
        for d in range(parts)
    ]
    far = full + 1
    kept = down_rows - units
    cut_by_shift = [jnp.concatenate([cut, gain_rows], axis=0) for cut in cuts]
    cut_by_shift[far] = jnp.concatenate([cuts[far][:kept], gain_rows], axis=0)
    one, three = parts - 1, parts - (far - 1)
    end = down_rows + 8
    first = shifted(jnp.concatenate([cut_by_shift[one], cuts[far][kept:]], axis=0), one)
    for d in range(1, parts):
        if d not in (one, three):
            cut_by_shift[d] = shifted(cut_by_shift[d], d)
    cut_by_shift[one] = first
    cut_by_shift[three] = shifted(
        jnp.concatenate([cut_by_shift[three], first[end:]], axis=0), three
    )
    turns = jnp.stack([(here - d + parts) % parts for d in range(parts)]).astype(jnp.int32)
    pieces = []
    for d, cut in enumerate(cut_by_shift):
        pieces.append((d, cut, 0, 0, kept if d == far else down_rows))
        pieces.append((d, cut, kept if d == far else down_rows, None, 8))
    pieces.append((far, cut_by_shift[three], end, kept, units))
    down_all, gains = unpacked(turns, pieces, parts, down_rows, width)

    placing, weights = route_tables(expert_ids, slot_ids, gate_num, rows_all)
    outgoing = lax.dot_general(
        placing, tokens, (((0,), (0,)), ((), ())), preferred_element_type=jnp.float32
    ).astype(jnp.bfloat16)
    received = sent(outgoing.reshape(sources, per_source, width), EXPERT)
    received = received.reshape(rows_all, width)

    size = rows_all // HALVES
    owner = (lax.broadcasted_iota(jnp.int32, (1, rows_all), 1)[0] % per_source) // CAP
    masks = [owner == e for e in range(local)]
    halves = [received[k * size : (k + 1) * size] for k in range(HALVES)]
    blocks = [{0: half} for half in halves]
    ahead, back = list(halves), list(halves)
    for s in range(1, full + 1):
        for k in range(HALVES):
            ahead[k] = blocks[k][s] = shifted(ahead[k], 1)
            back[k] = blocks[k][parts - s] = shifted(back[k], -1)
    early = [d for d in order if min(d, parts - d) < full]
    held = add_blocks(
        turns, gate_proj, up_proj, gains, {d: [b[d] for b in blocks] for d in early}, None, False
    )
    blocks[0][far] = shifted(ahead[0], 1)
    blocks[1][far] = shifted(back[1], -1)
    late = [d for d in order if d not in early]
    copies = add_blocks(
        turns, gate_proj, up_proj, gains, {d: [b[d] for b in blocks] for d in late}, held, True
    )
    held = (copies, down_all, weights, masks)
    copies, down_all, weights, masks = lax.optimization_barrier(held)
    gathered = sent(copies, "hidden")
    gathered = gathered.reshape(parts * units, rows_all)
    result = jnp.zeros((rows_all, width), jnp.float32)
    for e in range(local):
        spread = jnp.where(masks[e], gathered, jnp.zeros_like(gathered))
        down = down_all[:, e * units : (e + 1) * units].reshape(parts * units, width)
        result = result + lax.dot_general(
            spread, down, (((0,), (0,)), ((), ())), preferred_element_type=jnp.float32
        )

    tiles = result.astype(jnp.bfloat16).reshape(sources, per_source, width)
    returned = sent(tiles, EXPERT).reshape(rows_all, width)
    combined = jnp.dot(weights, returned, preferred_element_type=jnp.float32)
    return combined.astype(jnp.bfloat16)


def solution(mesh):
    torus = Mesh(
        mesh.devices.reshape(
            mesh.shape["groups"], mesh.shape["expert"] // 2, 2, mesh.shape["hidden"]
        ),
        ("groups", "expert_0", "expert_1", "hidden"),
    )
    in_specs = (
        P(GROUPS_EXPERT, "hidden"),
        P("hidden"),
        P(EXPERT, "hidden", None),
        P(EXPERT, "hidden", None),
        P(EXPERT, "hidden", None),
        P(GROUPS_EXPERT, None),
        P(GROUPS_EXPERT, None),
        P(GROUPS_EXPERT, None),
    )
    out_specs = P(GROUPS_EXPERT, "hidden")
    return jax.shard_map(layer, mesh=torus, in_specs=in_specs, out_specs=out_specs, check_vma=False)
```

```python
import jax
import jax.numpy as jnp
from jax import lax
from jax.experimental import pallas as pl
from jax.experimental.pallas import tpu as pltpu
from jax.sharding import Mesh
from jax.sharding import PartitionSpec as P

CAP = 12
HALVES = 2
LIMIT = 20 * 2**20
EXPERT = ("expert_0", "expert_1")
GROUPS_EXPERT = ("groups", "expert_0", "expert_1")


gate_scale = 1.0 / 1024.0


def shifted(array, step):
    devices = lax.axis_size("hidden")
    return lax.ppermute(array, "hidden", [(i, (i + step) % devices) for i in range(devices)])


def feature_block(weights, index, width):
    return lax.dynamic_slice_in_dim(weights, index * width, width, axis=weights.ndim - 1)


def sent(tiles, axes):
    return lax.all_to_all(tiles, axes, split_axis=0, concat_axis=0, tiled=True)


def route_tables(expert_ids, slot_ids, gate_num, slots):
    slot_index = expert_ids * CAP + slot_ids
    columns = lax.broadcasted_iota(jnp.int32, (1, 1, slots), 2)
    matches = slot_index[:, :, None] == columns
    placing = jnp.any(matches, axis=1).astype(jnp.bfloat16)
    scaled = gate_num.astype(jnp.float32) * gate_scale
    weights = jnp.sum(jnp.where(matches, scaled[:, :, None], 0.0), axis=1).astype(jnp.bfloat16)
    return (placing, weights)


def unpacked(turns, pieces, parts, rows, width):
    arrays = []
    for _, array, *_ in pieces:
        if not any(array is known for known in arrays):
            arrays.append(array)

    def place(array):
        return [array is known for known in arrays].index(True)

    def body(turn, *refs):
        sources, (down, sems) = refs[: len(arrays)], refs[len(arrays) :]
        moves = []
        for n, (d, array, low, at, count) in enumerate(pieces):
            target = down.at[turn[d], pl.ds(at, count)]
            source = sources[place(array)].at[pl.ds(low, count)]
            moves.append(pltpu.make_async_copy(source, target, sems.at[n]))
        for move in moves:
            move.start()
        for move in moves:
            move.wait()

    return pl.pallas_call(
        body,
        out_shape=jax.ShapeDtypeStruct((parts, rows, width), jnp.bfloat16),
        in_specs=[pl.BlockSpec(memory_space=pltpu.SMEM)]
        + [pl.BlockSpec(memory_space=pltpu.HBM)] * len(arrays),
        out_specs=pl.BlockSpec(memory_space=pltpu.VMEM),
        scratch_shapes=[pltpu.SemaphoreType.DMA((len(pieces),))],
        compiler_params=pltpu.CompilerParams(vmem_limit_bytes=LIMIT),
        cost_estimate=pl.CostEstimate(
            flops=10**8, bytes_accessed=4 * parts * rows * width, transcendentals=0
        ),
    )(turns, *arrays)


def add_blocks(turns, gate_proj, up_proj, gains, blocks, before, finish):
    local, units, features = gate_proj.shape
    count = len(blocks)
    pieces = [piece for group in blocks.values() for piece in group]
    width = pieces[0].shape[1]
    parts = features // width
    gain_from = [gains[d] for d in blocks]
    rows_all = sum(piece.shape[0] for piece in pieces) // count
    wide = 2 * local * units
    shapes = [
        jax.ShapeDtypeStruct((wide, rows_all), jnp.float32),
        jax.ShapeDtypeStruct((rows_all, 128), jnp.float32),
    ]

    def body(turn, gate, up, *refs):
        gain_refs, refs = refs[:count], refs[count:]
        block_refs, refs = refs[: len(pieces)], refs[len(pieces) :]
        refs, (landed, sems, gain_rows, gain_sems) = refs[:-4], refs[-4:]
        gain_moves = [
            pltpu.make_async_copy(ref.at[pl.ds(low, 8)], gain_rows.at[n], gain_sems.at[n])
            for n, (ref, (_, low)) in enumerate(zip(gain_refs, gain_from))
        ]
        moves = [
            pltpu.make_async_copy(ref, landed.at[n], sems.at[n]) for n, ref in enumerate(block_refs)
        ]
        for move in gain_moves + moves:
            move.start()
        done_pieces = 0
        start_sums, start_squares = refs[:2] if before else (None, None)
        refs = refs[2:] if before else refs
        out, (sums, squares) = (refs[0], refs[1:]) if finish else (None, refs)
        for n, (d, group) in enumerate(blocks.items()):
            start = pl.multiple_of(turn[d] * width, 128)
            cut = jnp.concatenate(
                [w[e, :, pl.ds(start, width)] for w in (gate, up) for e in range(local)], axis=0
            )
            gain_moves[n].wait()
            cut = cut * gain_rows[n, 0:1, :]
            first = 0
            for piece in group:
                moves[done_pieces].wait()
                rows = landed[done_pieces]
                done_pieces += 1
                here = pl.ds(first, piece.shape[0])
                first += piece.shape[0]
                product = lax.dot_general(
                    cut, rows, (((1,), (1,)), ((), ())), preferred_element_type=jnp.float32
                )
                square = jnp.square(rows.astype(jnp.float32))
                square = sum(square[:, k : k + 128] for k in range(0, width, 128))
                if n or before:
                    old_sums, old_squares = (sums, squares) if n else (start_sums, start_squares)
                    product = product + old_sums[:, here]
                    square = square + old_squares[here, :]
                sums[:, here] = product
                squares[here, :] = square
        if finish:
            total = jnp.sum(squares[...].T, axis=0, keepdims=True)
            scale = lax.rsqrt(total / features + 0.5)
            owner = lax.broadcasted_iota(jnp.int32, (1, rows_all), 1) % (local * CAP) // CAP
            own = []
            for k in range(2):
                value = sums[pl.ds(k * local * units, units), :]
                for e in range(1, local):
                    other = sums[pl.ds((k * local + e) * units, units), :]
                    value = jnp.where(owner == e, other, value)
                own.append(value * scale)
            done = (own[0] / (1.0 + jnp.exp(-own[0])) * own[1]).astype(jnp.bfloat16)
            for j in range(parts):
                out[j] = done

    vmem = pl.BlockSpec(memory_space=pltpu.VMEM)
    held = [] if before is None else list(before)
    done = jax.ShapeDtypeStruct((parts, units, rows_all), jnp.bfloat16)
    return pl.pallas_call(
        body,
        out_shape=done if finish else shapes,
        in_specs=[pl.BlockSpec(memory_space=pltpu.SMEM)]
        + [vmem] * 2
        + [pl.BlockSpec(memory_space=pltpu.HBM)] * (count + len(pieces))
        + [vmem] * len(held),
        out_specs=vmem if finish else [vmem] * 2,
        scratch_shapes=([pltpu.VMEM(s.shape, s.dtype) for s in shapes] if finish else [])
        + [
            pltpu.VMEM((len(pieces), *pieces[0].shape), pieces[0].dtype),
            pltpu.SemaphoreType.DMA((len(pieces),)),
            pltpu.VMEM((count, 8, width), pieces[0].dtype),
            pltpu.SemaphoreType.DMA((count,)),
        ],
        compiler_params=pltpu.CompilerParams(vmem_limit_bytes=LIMIT),
        cost_estimate=pl.CostEstimate(
            flops=2 * wide * width * rows_all * count, bytes_accessed=0, transcendentals=0
        ),
    )(turns, gate_proj, up_proj, *[array for array, _ in gain_from], *pieces, *held)


def layer(tokens, norm_gain, gate_proj, up_proj, down_proj, expert_ids, slot_ids, gate_num):
    parts = lax.axis_size("hidden")
    here = lax.axis_index("hidden")
    sources = lax.axis_size(EXPERT)
    local, units, _ = gate_proj.shape
    width = tokens.shape[1]
    per_source = local * CAP
    rows_all = sources * per_source
    down_rows = local * units

    full = (parts - 1) // 2
    order = [0]
    for s in range(1, full + 1):
        order += [s, parts - s]
    order.append(full + 1)

    gain_rows = jnp.broadcast_to(norm_gain[None, :], (8, width))
    cuts = [
        feature_block(down_proj, (here + d) % parts, width).reshape(down_rows, width)
        for d in range(parts)
    ]
    far = full + 1
    kept = down_rows - units
    cut_by_shift = [jnp.concatenate([cut, gain_rows], axis=0) for cut in cuts]
    cut_by_shift[far] = jnp.concatenate([cuts[far][:kept], gain_rows], axis=0)
    one, three = parts - 1, parts - (far - 1)
    end = down_rows + 8
    first = shifted(jnp.concatenate([cut_by_shift[one], cuts[far][kept:]], axis=0), one)
    for d in range(1, parts):
        if d not in (one, three):
            cut_by_shift[d] = shifted(cut_by_shift[d], d)
    cut_by_shift[one] = first
    cut_by_shift[three] = shifted(
        jnp.concatenate([cut_by_shift[three], first[end:]], axis=0), three
    )
    turns = jnp.stack([(here - d + parts) % parts for d in range(parts)]).astype(jnp.int32)
    pieces = [
        (d, cut, 0, 0, kept if d == far else down_rows) for d, cut in enumerate(cut_by_shift)
    ]
    pieces.append((far, cut_by_shift[three], end, kept, units))
    gains = [(cut, kept if d == far else down_rows) for d, cut in enumerate(cut_by_shift)]

    placing, weights = route_tables(expert_ids, slot_ids, gate_num, rows_all)
    outgoing = lax.dot_general(
        placing, tokens, (((0,), (0,)), ((), ())), preferred_element_type=jnp.float32
    ).astype(jnp.bfloat16)
    received = sent(outgoing.reshape(sources, per_source, width), EXPERT)
    received = received.reshape(rows_all, width)

    size = rows_all // HALVES
    owner = (lax.broadcasted_iota(jnp.int32, (1, rows_all), 1)[0] % per_source) // CAP
    masks = [owner == e for e in range(local)]
    halves = [received[k * size : (k + 1) * size] for k in range(HALVES)]
    blocks = [{0: half} for half in halves]
    ahead, back = list(halves), list(halves)
    for s in range(1, full + 1):
        for k in range(HALVES):
            ahead[k] = blocks[k][s] = shifted(ahead[k], 1)
            back[k] = blocks[k][parts - s] = shifted(back[k], -1)
    early = [d for d in order if min(d, parts - d) < full]
    held = add_blocks(
        turns, gate_proj, up_proj, gains, {d: [b[d] for b in blocks] for d in early}, None, False
    )
    blocks[0][far] = shifted(ahead[0], 1)
    blocks[1][far] = shifted(back[1], -1)
    late = [d for d in order if d not in early]
    copies = add_blocks(
        turns, gate_proj, up_proj, gains, {d: [b[d] for b in blocks] for d in late}, held, True
    )
    copies, weights, masks = lax.optimization_barrier((copies, weights, masks))
    turns, _ = lax.optimization_barrier((turns, copies))
    down_all = unpacked(turns, pieces, parts, down_rows, width)
    gathered = sent(copies, "hidden")
    gathered = gathered.reshape(parts * units, rows_all)
    result = jnp.zeros((rows_all, width), jnp.float32)
    for e in range(local):
        spread = jnp.where(masks[e], gathered, jnp.zeros_like(gathered))
        down = down_all[:, e * units : (e + 1) * units].reshape(parts * units, width)
        result = result + lax.dot_general(
            spread, down, (((0,), (0,)), ((), ())), preferred_element_type=jnp.float32
        )

    tiles = result.astype(jnp.bfloat16).reshape(sources, per_source, width)
    returned = sent(tiles, EXPERT).reshape(rows_all, width)
    combined = jnp.dot(weights, returned, preferred_element_type=jnp.float32)
    return combined.astype(jnp.bfloat16)


def solution(mesh):
    torus = Mesh(
        mesh.devices.reshape(
            mesh.shape["groups"], mesh.shape["expert"] // 2, 2, mesh.shape["hidden"]
        ),
        ("groups", "expert_0", "expert_1", "hidden"),
    )
    in_specs = (
        P(GROUPS_EXPERT, "hidden"),
        P("hidden"),
        P(EXPERT, "hidden", None),
        P(EXPERT, "hidden", None),
        P(EXPERT, "hidden", None),
        P(GROUPS_EXPERT, None),
        P(GROUPS_EXPERT, None),
        P(GROUPS_EXPERT, None),
    )
    out_specs = P(GROUPS_EXPERT, "hidden")
    return jax.shard_map(layer, mesh=torus, in_specs=in_specs, out_specs=out_specs, check_vma=False)
```
